32 devices in a mesh: orb: 8 (over y, x, core), walk: 4 (over z).
Axes of the slice: x: 2, y: 2, z: 4, core: 2. Of those that a mesh axis runs over, the one named last changes fastest.
Arguments:
- chol: bfloat16 [32, 2048, 2048], P(None, 'orb', 'walk'), may hold values from -6 to 6
- orbitals: bfloat16 [2048, 1024], replicated, may hold values from -0.125 to 0.125
- greens: bfloat16 [4, 1024, 2048], P('walk'), may hold values from -0.00390625 to 0.00390625
- shift: float32 [32], P('orb'), may hold values from -6 to 6
Outputs:
- force_bias: float32 [4, 32], P('walk', 'orb')
- rotated: bfloat16 [32, 1024, 2048], P('orb', None, 'walk')
The draws below stay inside these ranges and needn't reach their ends.
All inputs are finite; a program needn't handle non-finite values.
Results may differ from the reference program's by a relative error of at most 0.007.
Values may be sent and summed in bfloat16 or wider, within the bound.
A program may use at most 64 MiB of HBM per device.

```python
import jax
import jax.numpy as jnp
from jax import lax

N = 2048
NOCC = 1024
NV = 32
W = 4


def shard_levels(stream_key, shape, pieces, smallest, top_value):
    def one(dim, parts):
        heights = jax.random.uniform(jax.random.fold_in(jax.random.fold_in(stream_key, 6), dim), (parts,), jnp.float32, smallest / len(pieces), top_value / len(pieces))
        return jnp.repeat(jnp.exp(heights), shape[dim] // parts).reshape((-1,) + (1,) * (len(shape) - dim - 1))

    factor_of = one(*pieces[0])
    for cut in pieces[1:]:
        factor_of = factor_of * one(*cut)
    return factor_of


def normal_values(own_key, shape, width, limit, split=(), kind=jnp.bfloat16):
    loudness = shard_levels(own_key, shape, split, -0.22, 0.18) if split else 1.0
    result = jax.random.normal(own_key, shape, jnp.float32) * width * loudness
    return jnp.minimum(jnp.maximum(result, -limit), limit).astype(kind)


def setup_inputs(seed: int = 0) -> dict:
    key_list = jax.random.split(jax.random.key(seed), 5)
    chol = normal_values(key_list[0], (NV, N, N), 1.0, 6.0, ((1, 8), (2, 4)))
    orbitals = normal_values(key_list[1], (N, NOCC), N ** -0.5, 0.125)
    greens = normal_values(key_list[2], (W, NOCC, N), (NOCC * N) ** -0.5, 0.00390625, ((0, 4),))
    shift = normal_values(key_list[3], (NV,), 1.0, 6.0, ((0, 8),), jnp.float32)
    return dict(chol=chol, orbitals=orbitals, greens=greens, shift=shift)


def reference(chol, orbitals, greens, shift):
    flat_greens = greens.reshape(greens.shape[0], -1).astype(jnp.float32)
    orbitals_t = orbitals.T

    def one_vector(matrix):
        rotation = jnp.dot(orbitals_t, matrix, preferred_element_type=jnp.float32)
        column = jnp.dot(flat_greens, rotation.reshape(-1), precision=lax.Precision.HIGHEST)
        return rotation.astype(jnp.bfloat16), column

    rotated, columns = lax.map(one_vector, chol)
    force_bias = columns.T - shift[None, :]
    return (force_bias, rotated)
```

```python
import functools

import jax
import jax.numpy as jnp
from jax import lax
from jax.experimental import pallas as pl
from jax.experimental.pallas import tpu as pltpu
from jax.sharding import PartitionSpec as P

MESH = pl.DeviceIdType.MESH
LANES = 128


def xor(a, b, size):
    total, bit = 0, 1
    while bit < size:
        total = total + ((a // bit + b // bit) % 2) * bit
        bit *= 2
    return total


def low_bit(k):
    return k & -k


def ones(k):
    return bin(k).count("1")


def kernel(
    n, m, chol, orbitals, greens, shift, bias_out, rotated,
    chunks, first_v, chol_v, orb_v, orb_t, greens_v, products, arrived, acc,
    rows_v, terms, terms_in, sums, sums_in,
    local_sem, send_sem, recv_sem, walk_send, walk_recv,
    term_send, term_recv, sum_send, sum_recv, heard, chain,
):
    me, my_walk = lax.axis_index("orb"), lax.axis_index("walk")
    vectors, rows, cols = chol.shape
    owned = vectors // n
    walkers = greens.shape[0]
    half = n // 2
    leader = me == n - 1
    has_below, has_above = my_walk > 0, my_walk < m - 1
    bits = [1 << b for b in range(n.bit_length() - 1)]
    share = m * walkers * owned

    barrier = pltpu.get_barrier_semaphore()
    for bit in reversed(bits):
        pl.semaphore_signal(barrier, inc=1, device_id={"orb": xor(me, bit, n)}, device_id_type=MESH)

    def greet(other):
        pl.semaphore_signal(barrier, inc=1, device_id={"walk": other}, device_id_type=MESH)

    pl.when(leader & has_below)(lambda: greet(my_walk - 1))
    pl.when(leader & has_above)(lambda: greet(my_walk + 1))

    firsts = [
        pltpu.make_async_copy(chol.at[xor(me, bit, n) * owned], first_v.at[i], local_sem.at[3 + i])
        for i, bit in enumerate(bits[1:])
    ]
    for load in firsts:
        load.start()
    loads = [
        pltpu.make_async_copy(greens, greens_v, local_sem.at[0]),
        pltpu.make_async_copy(orbitals, orb_v, local_sem.at[1]),
        pltpu.make_async_copy(chol, chol_v, local_sem.at[2]),
    ]

    planes = (my_walk + m - 1) // m + (2 * m - 2 - my_walk) // m
    pl.semaphore_wait(barrier, len(bits) + me // (n - 1) * planes)

    def tell(k):
        peer = xor(me, low_bit(k), n)
        pl.semaphore_signal(heard.at[k], inc=1, device_id={"orb": peer}, device_id_type=MESH)

    def hear(k):
        if ones(k) > 1:
            pl.semaphore_wait(heard.at[k], 1)
        for further in range(k + 1, n):
            if ones(further) == ones(k) + 1 and further - low_bit(further) == k:
                tell(further)

    for bit in bits:
        hear(bit)

    def chunk_copy(g, k, src=None):
        peer = xor(me, k, n)
        return pltpu.make_async_remote_copy(
            src_ref=chol.at[peer * owned + g] if src is None else src,
            dst_ref=chunks.at[k, g],
            send_sem=send_sem.at[k, g],
            recv_sem=recv_sem.at[k, g],
            device_id={"orb": peer},
            device_id_type=MESH,
        )

    def send_vector(g):
        for low in range(2):
            if low == 1:
                chunk_copy(g, 1).start()
            for chip in range(half - 1, 0, -1):
                chunk_copy(g, chip * 2 + low).start()

    for i, bit in enumerate(bits[1:]):
        firsts[i].wait()
        chunk_copy(0, bit, first_v.at[i]).start()
    chunk_copy(0, 1).start()
    for low in range(2):
        for k in range(2 + low, n, 2):
            if ones(k) > 1:
                hear(k)
                chunk_copy(0, k).start()
    early = max(owned - 1, 1)
    for g in range(1, early):
        send_vector(g)

    for load in loads:
        load.start()

    def pass_on(i, other):
        pl.semaphore_signal(chain.at[i], inc=1, device_id={"walk": other}, device_id_type=MESH)

    pl.when(leader & has_below)(lambda: pl.semaphore_wait(chain.at[0], 1))
    pl.when(leader & has_above)(lambda: pass_on(0, my_walk + 1))
    pl.when(leader & has_above)(lambda: pl.semaphore_wait(chain.at[1], 1))
    pl.when(leader & has_below)(lambda: pass_on(1, my_walk - 1))

    @pl.when(leader)
    def _():
        for k in range(1, n):
            pl.semaphore_signal(
                chain.at[2], inc=1, device_id={"orb": xor(me, k, n)}, device_id_type=MESH
            )

    loads[0].wait()
    loads[1].wait()
    my_rows = orb_v[pl.ds(pl.multiple_of(me * rows, rows), rows), :]
    for w in range(walkers):
        for j in range(m):
            products[j, w] = jnp.dot(
                my_rows, greens_v[w, :, j * cols : (j + 1) * cols],
                preferred_element_type=jnp.float32,
            ).astype(products.dtype)

    def turn(s, _):
        orb_t[s] = orb_v[pl.ds(pl.multiple_of(s * rows, rows), rows), :].T
        return _

    lax.fori_loop(0, n, turn, 0)

    def walk_copy(k):
        peer = (my_walk + k) % m
        return pltpu.make_async_remote_copy(
            src_ref=products.at[peer],
            dst_ref=arrived.at[m - k],
            send_sem=walk_send.at[k],
            recv_sem=walk_recv.at[m - k],
            device_id={"walk": peer},
            device_id_type=MESH,
        )

    def walk_arrival(k):
        return pltpu.make_async_remote_copy(
            src_ref=products.at[0],
            dst_ref=arrived.at[k],
            send_sem=walk_send.at[k],
            recv_sem=walk_recv.at[k],
            device_id={"walk": (my_walk + k) % m},
            device_id_type=MESH,
        )

    pl.when(me < n - 1)(lambda: pl.semaphore_wait(chain.at[2], 1))
    for k in range(1, m):
        walk_copy(k).start()

    loads[2].wait()

    def begin(g, _):
        acc[g] = jnp.dot(orb_t[me], chol_v[me * owned + g], preferred_element_type=jnp.float32)
        return _

    lax.fori_loop(0, owned, begin, 0)
    arrived[0] = products[my_walk]
    for k in range(1, m):
        walk_arrival(k).wait_recv()

    def term(v, _):
        block = chol_v[v].astype(jnp.float32)
        start = (v // owned) * share + v % owned
        for k in range(m):
            from_walk = (my_walk + k) % m
            for w in range(walkers):
                both = block * arrived[k, w].astype(jnp.float32)
                both = jnp.sum(both, axis=0, keepdims=True)
                part = both[:, :LANES]
                for lane in range(LANES, cols, LANES):
                    part = part + both[:, lane : lane + LANES]
                rows_v[pl.ds(start + (from_walk * walkers + w) * owned, 1), :] = part
        return _

    lax.fori_loop(0, vectors, term, 0)
    for b in range(terms.shape[0]):
        turned = rows_v[b * LANES : (b + 1) * LANES, :].T
        terms[b] = jnp.sum(turned, axis=0, keepdims=True)

    def take(g, k):
        chunk_copy(g, k).wait_recv()
        return acc[g] + jnp.dot(
            orb_t[xor(me, k, n)], chunks[k, g], preferred_element_type=jnp.float32
        )

    def arrival(i):
        return (half - 1 - i % (half - 1)) * 2 + i // (half - 1)

    steps = 2 * (half - 1)

    def add(g, k):
        acc[g] = take(g, k)

    def add_some(g, start, stop):
        def step(i, _):
            add(g, arrival(i))
            return _

        lax.fori_loop(start, stop, step, 0)

    def finish(g):
        rotated[g] = take(g, arrival(steps - 1)).astype(rotated.dtype)

    def term_copy(k):
        peer = xor(me, k, n)
        return pltpu.make_async_remote_copy(
            src_ref=terms.at[peer * share // LANES],
            dst_ref=terms_in.at[k],
            send_sem=term_send.at[k],
            recv_sem=term_recv.at[k],
            device_id={"orb": peer},
            device_id_type=MESH,
        )

    def sum_copy(k):
        peer = (my_walk + k) % m
        return pltpu.make_async_remote_copy(
            src_ref=sums,
            dst_ref=sums_in.at[m - k],
            send_sem=sum_send.at[k],
            recv_sem=sum_recv.at[m - k],
            device_id={"walk": peer},
            device_id_type=MESH,
        )

    def sum_arrival(k):
        return pltpu.make_async_remote_copy(
            src_ref=sums,
            dst_ref=sums_in.at[k],
            send_sem=sum_send.at[k],
            recv_sem=sum_recv.at[k],
            device_id={"walk": (my_walk + k) % m},
            device_id_type=MESH,
        )

    add(0, 1)
    add_some(0, 0, steps - 1)
    for k in range(1, n):
        term_copy(k).start()
    for g in range(early, owned):
        send_vector(g)
    if owned > 1:
        finish(0)

    if owned > 2:
        def vector(g, _):
            add(g, 1)
            add_some(g, 0, steps - 1)
            finish(g)
            return _

        lax.fori_loop(1, owned - 1, vector, 0)

    def drain(g, _):
        def one(k, _):
            chunk_copy(g, k).wait_send()
            return _

        return lax.fori_loop(1, n, one, _)

    last = owned - 1
    lax.fori_loop(0, last, drain, 0)
    for k in range(1, m):
        walk_copy(k).wait_send()
    for k in range(1, n):
        term_copy(k).wait_send()

    mine = terms[me * share // LANES]
    for k in range(1, n):
        term_copy(k).wait_recv()
        mine = mine + terms_in[k]
    sums[...] = mine
    if owned > 1:
        add(last, 1)
    for k in range(1, m):
        sum_copy(k).start()
    if owned > 1:
        add_some(last, 0, steps - 2)
    total = sums[...]
    for k in range(1, m):
        sum_arrival(k).wait_recv()
        total = total + sums_in[k]
    offset = (me * share) % LANES + my_walk * (walkers * owned)
    total = pltpu.roll(jnp.broadcast_to(total, (8, LANES)), (LANES - offset) % LANES, 1)
    for w in range(walkers):
        bias_out[w : w + 1, :] = total[:1, w * owned : (w + 1) * owned] - shift[...]
    for k in range(1, m):
        sum_copy(k).wait_send()
    if owned > 1:
        add_some(last, steps - 2, steps - 1)
    finish(last)
    drain(last, 0)


def store(bias, rounded, bias_out, rotated, sems):
    owned = rounded.shape[0]
    writes = [
        pltpu.make_async_copy(rounded.at[g], rotated.at[g], sems.at[g]) for g in range(owned)
    ]
    writes.append(pltpu.make_async_copy(bias, bias_out, sems.at[owned]))
    for write in writes:
        write.start()
    for write in writes:
        write.wait()


def local(n, m, chol, orbitals, greens, shift):
    vectors, rows, cols = chol.shape
    owned = vectors // n
    walkers, occupied, _ = greens.shape
    bf16, f32 = jnp.bfloat16, jnp.float32
    dma = pltpu.SemaphoreType.DMA
    regular = pltpu.SemaphoreType.REGULAR
    any_space = pl.BlockSpec(memory_space=pl.ANY)
    vmem = pl.BlockSpec(memory_space=pltpu.VMEM)
    singles = n.bit_length() - 2
    packed = n * m * walkers * owned // LANES
    bias, rounded = pl.pallas_call(
        functools.partial(kernel, n, m),
        out_shape=(
            pltpu.VMEM((walkers, owned), f32),
            pltpu.VMEM((owned, occupied, cols), bf16),
        ),
        in_specs=[any_space] * 3 + [vmem],
        out_specs=(vmem, vmem),
        scratch_shapes=[
            pltpu.VMEM((n, owned, rows, cols), bf16),
            pltpu.VMEM((singles, rows, cols), bf16),
            pltpu.VMEM(chol.shape, bf16),
            pltpu.VMEM(orbitals.shape, bf16),
            pltpu.VMEM((n, occupied, rows), bf16),
            pltpu.VMEM(greens.shape, bf16),
            pltpu.VMEM((m, walkers, rows, cols), bf16),
            pltpu.VMEM((m, walkers, rows, cols), bf16),
            pltpu.VMEM((owned, occupied, cols), f32),
            pltpu.VMEM((packed * LANES, LANES), f32),
            pltpu.VMEM((packed, 1, LANES), f32),
            pltpu.VMEM((n, 1, LANES), f32),
            pltpu.VMEM((1, LANES), f32),
            pltpu.VMEM((m, 1, LANES), f32),
            dma((3 + singles,)),
            dma((n, owned)),
            dma((n, owned)),
            dma((m,)),
            dma((m,)),
            dma((n,)),
            dma((n,)),
            dma((m,)),
            dma((m,)),
            regular((n,)),
            regular((3,)),
        ],
        compiler_params=pltpu.CompilerParams(
            collective_id=0, has_side_effects=True, vmem_limit_bytes=59 * 2**20
        ),
    )(chol, orbitals, greens, shift.reshape(1, owned))
    return pl.pallas_call(
        store,
        out_shape=(
            jax.ShapeDtypeStruct((walkers, owned), f32),
            jax.ShapeDtypeStruct((owned, occupied, cols), bf16),
        ),
        in_specs=[vmem, vmem],
        out_specs=(any_space, any_space),
        scratch_shapes=[dma((owned + 1,))],
        compiler_params=pltpu.CompilerParams(vmem_limit_bytes=2**20),
    )(bias, rounded)


def solution(mesh):
    in_specs = (P(None, "orb", "walk"), P(), P("walk", None, None), P("orb"))
    out_specs = (P("walk", "orb"), P("orb", None, "walk"))
    body = functools.partial(local, mesh.shape["orb"], mesh.shape["walk"])
    return jax.shard_map(body, mesh=mesh, in_specs=in_specs, out_specs=out_specs, check_vma=False)
```

```python
import functools

import jax
import jax.numpy as jnp
from jax import lax
from jax.experimental import pallas as pl
from jax.experimental.pallas import tpu as pltpu
from jax.sharding import PartitionSpec as P

MESH = pl.DeviceIdType.MESH
LANES = 128


def xor(a, b, size):
    total, bit = 0, 1
    while bit < size:
        total = total + ((a // bit + b // bit) % 2) * bit
        bit *= 2
    return total


def low_bit(k):
    return k & -k


def ones(k):
    return bin(k).count("1")


def kernel(
    n, m, chol, orbitals, greens, shift,
    bias_out, rounded, acc_last, chunk_last, orb_last,
    chunks, first_v, chol_v, orb_v, orb_t, greens_v, products, arrived, acc,
    rows_v, terms, terms_in, sums, sums_in, shift_v,
    local_sem, send_sem, recv_sem, walk_send, walk_recv,
    term_send, term_recv, sum_send, sum_recv, heard, chain,
):
    me, my_walk = lax.axis_index("orb"), lax.axis_index("walk")
    vectors, rows, cols = chol.shape
    owned = vectors // n
    walkers = greens.shape[0]
    half = n // 2
    leader = me == n - 1
    has_below, has_above = my_walk > 0, my_walk < m - 1
    bits = [1 << b for b in range(n.bit_length() - 1)]
    share = m * walkers * owned

    barrier = pltpu.get_barrier_semaphore()
    for bit in reversed(bits):
        pl.semaphore_signal(barrier, inc=1, device_id={"orb": xor(me, bit, n)}, device_id_type=MESH)

    def greet(other):
        pl.semaphore_signal(barrier, inc=1, device_id={"walk": other}, device_id_type=MESH)

    pl.when(leader & has_below)(lambda: greet(my_walk - 1))
    pl.when(leader & has_above)(lambda: greet(my_walk + 1))

    firsts = [
        pltpu.make_async_copy(chol.at[xor(me, bit, n) * owned], first_v.at[i], local_sem.at[4 + i])
        for i, bit in enumerate(bits[1:])
    ]
    for load in firsts:
        load.start()
    loads = [
        pltpu.make_async_copy(greens, greens_v, local_sem.at[0]),
        pltpu.make_async_copy(orbitals, orb_v, local_sem.at[1]),
        pltpu.make_async_copy(chol, chol_v, local_sem.at[2]),
        pltpu.make_async_copy(shift, shift_v, local_sem.at[3]),
    ]

    planes = (my_walk + m - 1) // m + (2 * m - 2 - my_walk) // m
    pl.semaphore_wait(barrier, len(bits) + me // (n - 1) * planes)

    def tell(k):
        peer = xor(me, low_bit(k), n)
        pl.semaphore_signal(heard.at[k], inc=1, device_id={"orb": peer}, device_id_type=MESH)

    def hear(k):
        if ones(k) > 1:
            pl.semaphore_wait(heard.at[k], 1)
        for further in range(k + 1, n):
            if ones(further) == ones(k) + 1 and further - low_bit(further) == k:
                tell(further)

    for bit in bits:
        hear(bit)

    last, final = owned - 1, 3

    def chunk_copy(g, k, src=None, dst=None):
        peer = xor(me, k, n)
        return pltpu.make_async_remote_copy(
            src_ref=chol.at[peer * owned + g] if src is None else src,
            dst_ref=chunks.at[k, g] if dst is None else dst,
            send_sem=send_sem.at[k, g],
            recv_sem=recv_sem.at[k, g],
            device_id={"orb": peer},
            device_id_type=MESH,
        )

    def send_vector(g):
        for low in range(2):
            if low == 1:
                chunk_copy(g, 1).start()
            for chip in range(half - 1, 0, -1):
                k = chip * 2 + low
                chunk_copy(g, k, dst=chunk_last if (g, k) == (last, final) else None).start()

    for i, bit in enumerate(bits[1:]):
        firsts[i].wait()
        chunk_copy(0, bit, first_v.at[i]).start()
    chunk_copy(0, 1).start()
    for low in range(2):
        for k in range(2 + low, n, 2):
            if ones(k) > 1:
                hear(k)
                chunk_copy(0, k).start()
    early = max(owned - 1, 1)
    for g in range(1, early):
        send_vector(g)

    for load in loads:
        load.start()

    def pass_on(i, other):
        pl.semaphore_signal(chain.at[i], inc=1, device_id={"walk": other}, device_id_type=MESH)

    pl.when(leader & has_below)(lambda: pl.semaphore_wait(chain.at[0], 1))
    pl.when(leader & has_above)(lambda: pass_on(0, my_walk + 1))
    pl.when(leader & has_above)(lambda: pl.semaphore_wait(chain.at[1], 1))
    pl.when(leader & has_below)(lambda: pass_on(1, my_walk - 1))

    @pl.when(leader)
    def _():
        for k in range(1, n):
            pl.semaphore_signal(
                chain.at[2], inc=1, device_id={"orb": xor(me, k, n)}, device_id_type=MESH
            )

    loads[0].wait()
    loads[1].wait()
    my_rows = orb_v[pl.ds(pl.multiple_of(me * rows, rows), rows), :]
    for w in range(walkers):
        for j in range(m):
            products[j, w] = jnp.dot(
                my_rows, greens_v[w, :, j * cols : (j + 1) * cols],
                preferred_element_type=jnp.float32,
            ).astype(products.dtype)

    def turn(s, _):
        orb_t[s] = orb_v[pl.ds(pl.multiple_of(s * rows, rows), rows), :].T
        return _

    lax.fori_loop(0, n, turn, 0)
    orb_last[...] = orb_t[xor(me, final, n)]

    def walk_copy(k):
        peer = (my_walk + k) % m
        return pltpu.make_async_remote_copy(
            src_ref=products.at[peer],
            dst_ref=arrived.at[m - k],
            send_sem=walk_send.at[k],
            recv_sem=walk_recv.at[m - k],
            device_id={"walk": peer},
            device_id_type=MESH,
        )

    def walk_arrival(k):
        return pltpu.make_async_remote_copy(
            src_ref=products.at[0],
            dst_ref=arrived.at[k],
            send_sem=walk_send.at[k],
            recv_sem=walk_recv.at[k],
            device_id={"walk": (my_walk + k) % m},
            device_id_type=MESH,
        )

    pl.when(me < n - 1)(lambda: pl.semaphore_wait(chain.at[2], 1))
    for k in range(1, m):
        walk_copy(k).start()

    loads[2].wait()

    def begin(g, _):
        acc[g] = jnp.dot(orb_t[me], chol_v[me * owned + g], preferred_element_type=jnp.float32)
        return _

    lax.fori_loop(0, last, begin, 0)
    acc_last[...] = jnp.dot(
        orb_t[me], chol_v[me * owned + last], preferred_element_type=jnp.float32
    )
    arrived[0] = products[my_walk]
    for k in range(1, m):
        walk_arrival(k).wait_recv()

    def term(v, _):
        block = chol_v[v].astype(jnp.float32)
        start = (v // owned) * share + v % owned
        for k in range(m):
            from_walk = (my_walk + k) % m
            for w in range(walkers):
                both = block * arrived[k, w].astype(jnp.float32)
                both = jnp.sum(both, axis=0, keepdims=True)
                part = both[:, :LANES]
                for lane in range(LANES, cols, LANES):
                    part = part + both[:, lane : lane + LANES]
                rows_v[pl.ds(start + (from_walk * walkers + w) * owned, 1), :] = part
        return _

    lax.fori_loop(0, vectors, term, 0)
    for b in range(terms.shape[0]):
        turned = rows_v[b * LANES : (b + 1) * LANES, :].T
        terms[b] = jnp.sum(turned, axis=0, keepdims=True)

    def take(g, k):
        chunk_copy(g, k).wait_recv()
        return jnp.dot(orb_t[xor(me, k, n)], chunks[k, g], preferred_element_type=jnp.float32)

    def arrival(i):
        return (half - 1 - i % (half - 1)) * 2 + i // (half - 1)

    steps = 2 * (half - 1)

    def add(g, k):
        if isinstance(g, int) and g == last:
            acc_last[...] += take(g, k)
        else:
            acc[g] += take(g, k)

    def add_some(g, start, stop):
        def step(i, _):
            add(g, arrival(i))
            return _

        lax.fori_loop(start, stop, step, 0)

    def finish(g):
        rounded[g] = (acc[g] + take(g, arrival(steps - 1))).astype(rounded.dtype)

    def term_copy(k):
        peer = xor(me, k, n)
        return pltpu.make_async_remote_copy(
            src_ref=terms.at[peer * share // LANES],
            dst_ref=terms_in.at[k],
            send_sem=term_send.at[k],
            recv_sem=term_recv.at[k],
            device_id={"orb": peer},
            device_id_type=MESH,
        )

    def sum_copy(k):
        peer = (my_walk + k) % m
        return pltpu.make_async_remote_copy(
            src_ref=sums,
            dst_ref=sums_in.at[m - k],
            send_sem=sum_send.at[k],
            recv_sem=sum_recv.at[m - k],
            device_id={"walk": peer},
            device_id_type=MESH,
        )

    def sum_arrival(k):
        return pltpu.make_async_remote_copy(
            src_ref=sums,
            dst_ref=sums_in.at[k],
            send_sem=sum_send.at[k],
            recv_sem=sum_recv.at[k],
            device_id={"walk": (my_walk + k) % m},
            device_id_type=MESH,
        )

    add(0, 1)
    add_some(0, 0, steps - 1)
    for k in range(1, n):
        term_copy(k).start()
    for g in range(early, owned):
        send_vector(g)
    if owned > 1:
        finish(0)

    if owned > 2:
        def vector(g, _):
            add(g, 1)
            add_some(g, 0, steps - 1)
            finish(g)
            return _

        lax.fori_loop(1, owned - 1, vector, 0)

    def drain(g, _):
        def one(k, _):
            chunk_copy(g, k).wait_send()
            return _

        return lax.fori_loop(1, n, one, _)

    lax.fori_loop(0, last, drain, 0)
    for k in range(1, m):
        walk_copy(k).wait_send()
    for k in range(1, n):
        term_copy(k).wait_send()

    mine = terms[me * share // LANES]
    for k in range(1, n):
        term_copy(k).wait_recv()
        mine = mine + terms_in[k]
    sums[...] = mine
    if owned > 1:
        add(last, 1)
    for k in range(1, m):
        sum_copy(k).start()
    if owned > 1:
        add_some(last, 0, steps - 2)
    loads[3].wait()
    total = sums[...]
    for k in range(1, m):
        sum_arrival(k).wait_recv()
        total = total + sums_in[k]
    offset = (me * share) % LANES + my_walk * (walkers * owned)
    total = pltpu.roll(jnp.broadcast_to(total, (8, LANES)), (LANES - offset) % LANES, 1)
    for w in range(walkers):
        bias_out[w : w + 1, :] = total[:1, w * owned : (w + 1) * owned] - shift_v[...]
    for k in range(1, m):
        sum_copy(k).wait_send()
    if owned > 1:
        add_some(last, steps - 2, steps - 1)
    chunk_copy(last, final, dst=chunk_last).wait_recv()
    drain(last, 0)


def store(bias, rounded, acc_last, chunk_last, orb_last, bias_out, rotated, last_v, sems):
    last = rounded.shape[0]
    writes = [pltpu.make_async_copy(rounded.at[g], rotated.at[g], sems.at[g]) for g in range(last)]
    writes.append(pltpu.make_async_copy(last_v, rotated.at[last], sems.at[last]))
    writes.append(pltpu.make_async_copy(bias, bias_out, sems.at[last + 1]))
    for write in writes[:last]:
        write.start()
    last_v[...] = (
        acc_last[...]
        + jnp.dot(orb_last[...], chunk_last[...], preferred_element_type=jnp.float32)
    ).astype(last_v.dtype)
    for write in writes[last:]:
        write.start()
    for write in writes:
        write.wait()


def local(n, m, chol, orbitals, greens, shift):
    vectors, rows, cols = chol.shape
    owned = vectors // n
    walkers, occupied, _ = greens.shape
    bf16, f32 = jnp.bfloat16, jnp.float32
    dma = pltpu.SemaphoreType.DMA
    regular = pltpu.SemaphoreType.REGULAR
    any_space = pl.BlockSpec(memory_space=pl.ANY)
    vmem = pl.BlockSpec(memory_space=pltpu.VMEM)
    singles = n.bit_length() - 2
    packed = n * m * walkers * owned // LANES
    carried = pl.pallas_call(
        functools.partial(kernel, n, m),
        out_shape=(
            pltpu.VMEM((walkers, owned), f32),
            pltpu.VMEM((owned - 1, occupied, cols), bf16),
            pltpu.VMEM((occupied, cols), f32),
            pltpu.VMEM((rows, cols), bf16),
            pltpu.VMEM((occupied, rows), bf16),
        ),
        in_specs=[any_space] * 4,
        out_specs=(vmem,) * 5,
        scratch_shapes=[
            pltpu.VMEM((n, owned, rows, cols), bf16),
            pltpu.VMEM((singles, rows, cols), bf16),
            pltpu.VMEM(chol.shape, bf16),
            pltpu.VMEM(orbitals.shape, bf16),
            pltpu.VMEM((n, occupied, rows), bf16),
            pltpu.VMEM(greens.shape, bf16),
            pltpu.VMEM((m, walkers, rows, cols), bf16),
            pltpu.VMEM((m, walkers, rows, cols), bf16),
            pltpu.VMEM((owned - 1, occupied, cols), f32),
            pltpu.VMEM((packed * LANES, LANES), f32),
            pltpu.VMEM((packed, 1, LANES), f32),
            pltpu.VMEM((n, 1, LANES), f32),
            pltpu.VMEM((1, LANES), f32),
            pltpu.VMEM((m, 1, LANES), f32),
            pltpu.VMEM((1, owned), f32),
            dma((4 + singles,)),
            dma((n, owned)),
            dma((n, owned)),
            dma((m,)),
            dma((m,)),
            dma((n,)),
            dma((n,)),
            dma((m,)),
            dma((m,)),
            regular((n,)),
            regular((3,)),
        ],
        compiler_params=pltpu.CompilerParams(
            collective_id=0, has_side_effects=True, vmem_limit_bytes=56 * 2**20
        ),
    )(chol, orbitals, greens, shift.reshape(1, owned))
    return pl.pallas_call(
        store,
        out_shape=(
            jax.ShapeDtypeStruct((walkers, owned), f32),
            jax.ShapeDtypeStruct((owned, occupied, cols), bf16),
        ),
        in_specs=[vmem] * 5,
        out_specs=(any_space, any_space),
        scratch_shapes=[pltpu.VMEM((occupied, cols), bf16), dma((owned + 1,))],
        compiler_params=pltpu.CompilerParams(vmem_limit_bytes=8 * 2**20),
    )(*carried)


def solution(mesh):
    in_specs = (P(None, "orb", "walk"), P(), P("walk", None, None), P("orb"))
    out_specs = (P("walk", "orb"), P("orb", None, "walk"))
    body = functools.partial(local, mesh.shape["orb"], mesh.shape["walk"])
    return jax.shard_map(body, mesh=mesh, in_specs=in_specs, out_specs=out_specs, check_vma=False)
```

```python
import functools

import jax
import jax.numpy as jnp
from jax import lax
from jax.experimental import pallas as pl
from jax.experimental.pallas import tpu as pltpu
from jax.sharding import PartitionSpec as P

MESH = pl.DeviceIdType.MESH
LANES = 128


def xor(a, b, size):
    total, bit = 0, 1
    while bit < size:
        total = total + ((a // bit + b // bit) % 2) * bit
        bit *= 2
    return total


def low_bit(k):
    return k & -k


def ones(k):
    return bin(k).count("1")


def kernel(
    n, m, chol, orbitals, greens, shift,
    bias_out, rounded, acc_last, chunk_last, orb_last,
    chunks, first_v, chol_v, orb_v, orb_t, greens_v, products, arrived, acc,
    rows_v, terms, terms_in, sums, sums_in, shift_v,
    local_sem, send_sem, recv_sem, walk_send, walk_recv,
    term_send, term_recv, sum_send, sum_recv, heard, chain,
):
    me, my_walk = lax.axis_index("orb"), lax.axis_index("walk")
    vectors, rows, cols = chol.shape
    owned = vectors // n
    walkers = greens.shape[0]
    half = n // 2
    core = me % 2
    last, final = owned - 1, 3
    leader = me == n - 1
    has_below, has_above = my_walk > 0, my_walk < m - 1
    bits = [1 << b for b in range(n.bit_length() - 1)]
    share = m * walkers * owned

    def is_set(bit):
        return (me // bit) % 2

    barrier = pltpu.get_barrier_semaphore()

    def greet_orb(bit):
        pl.semaphore_signal(barrier, inc=1, device_id={"orb": xor(me, bit, n)}, device_id_type=MESH)

    for bit in reversed(bits[1:]):
        pl.when(is_set(bit) == 0)(functools.partial(greet_orb, bit))
    greet_orb(1)

    def greet(other):
        pl.semaphore_signal(barrier, inc=1, device_id={"walk": other}, device_id_type=MESH)

    pl.when(leader & has_below)(lambda: greet(my_walk - 1))
    pl.when(leader & has_above)(lambda: greet(my_walk + 1))

    firsts = [
        pltpu.make_async_copy(chol.at[xor(me, bit, n) * owned], first_v.at[i], local_sem.at[4 + i])
        for i, bit in enumerate(bits[1:])
    ]
    for load in firsts:
        load.start()
    loads = [
        pltpu.make_async_copy(chol, chol_v, local_sem.at[0]),
        pltpu.make_async_copy(orbitals, orb_v, local_sem.at[1]),
        pltpu.make_async_copy(greens, greens_v, local_sem.at[2]),
        pltpu.make_async_copy(shift, shift_v, local_sem.at[3]),
    ]

    planes = (my_walk + m - 1) // m + (2 * m - 2 - my_walk) // m
    pl.semaphore_wait(barrier, 1 + sum(is_set(bit) for bit in bits[1:]) + me // (n - 1) * planes)

    def chunk_copy(g, k, src=None, dst=None):
        peer = xor(me, k, n)
        source = chol if isinstance(g, int) and g == 0 else chol_v
        return pltpu.make_async_remote_copy(
            src_ref=source.at[peer * owned + g] if src is None else src,
            dst_ref=chunks.at[k, g] if dst is None else dst,
            send_sem=send_sem.at[k, g],
            recv_sem=recv_sem.at[k, g],
            device_id={"orb": peer},
            device_id_type=MESH,
        )

    def send_vector(g):
        for low in range(2):
            if low == 1:
                chunk_copy(g, 1).start()
            for high in range(1, half):
                if g == last and low == 1:
                    k = (half - high) * 2 + low
                    chunk_copy(g, k, dst=chunk_last if k == final else None).start()
                else:
                    chunk_copy(g, (high + core * (half - 2 * high)) * 2 + low).start()

    def tell(k):
        peer = xor(me, low_bit(k), n)
        pl.semaphore_signal(heard.at[k], inc=1, device_id={"orb": peer}, device_id_type=MESH)

    def hear(k):
        pl.semaphore_wait(heard.at[k], 1)

    def pass_along(k):
        for further in range(k + 1, n):
            if ones(further) == ones(k) + 1 and further - low_bit(further) == k:
                tell(further)

    def send_first(i, bit):
        firsts[i].wait()
        chunk_copy(0, bit, first_v.at[i]).start()

    for bit in reversed(bits[1:]):
        pl.when(is_set(bit) == 1)(functools.partial(tell, bit))
    for i, bit in enumerate(bits[1:]):
        pl.when(is_set(bit) == 1)(functools.partial(send_first, i, bit))
    for i, bit in enumerate(bits[1:]):
        pl.when(is_set(bit) == 0)(functools.partial(hear, bit))
        pl.when(is_set(bit) == 0)(functools.partial(send_first, i, bit))
        pass_along(bit)
    chunk_copy(0, 1).start()
    for low in range(2):
        for k in range(2 + low, n, 2):
            if ones(k) > 1:
                hear(k)
                pass_along(k)
                chunk_copy(0, k).start()
    for load in loads:
        load.start()
    loads[0].wait()
    for g in range(1, last):
        send_vector(g)

    def pass_on(i, other):
        pl.semaphore_signal(chain.at[i], inc=1, device_id={"walk": other}, device_id_type=MESH)

    pl.when(leader & has_below)(lambda: pl.semaphore_wait(chain.at[0], 1))
    pl.when(leader & has_above)(lambda: pass_on(0, my_walk + 1))
    pl.when(leader & has_above)(lambda: pl.semaphore_wait(chain.at[1], 1))
    pl.when(leader & has_below)(lambda: pass_on(1, my_walk - 1))

    @pl.when(leader)
    def _():
        for k in range(1, n):
            pl.semaphore_signal(
                chain.at[2], inc=1, device_id={"orb": xor(me, k, n)}, device_id_type=MESH
            )

    loads[1].wait()
    loads[2].wait()
    my_rows = orb_v[pl.ds(pl.multiple_of(me * rows, rows), rows), :]
    for w in range(walkers):
        for j in range(m):
            products[j, w] = jnp.dot(
                my_rows, greens_v[w, :, j * cols : (j + 1) * cols],
                preferred_element_type=jnp.float32,
            ).astype(products.dtype)

    def turn(s, _):
        orb_t[s] = orb_v[pl.ds(pl.multiple_of(s * rows, rows), rows), :].T
        return _

    lax.fori_loop(0, n, turn, 0)
    orb_last[...] = orb_t[xor(me, final, n)]

    def walk_copy(k):
        peer = (my_walk + k) % m
        return pltpu.make_async_remote_copy(
            src_ref=products.at[peer],
            dst_ref=arrived.at[m - k],
            send_sem=walk_send.at[k],
            recv_sem=walk_recv.at[m - k],
            device_id={"walk": peer},
            device_id_type=MESH,
        )

    def walk_arrival(k):
        return pltpu.make_async_remote_copy(
            src_ref=products.at[0],
            dst_ref=arrived.at[k],
            send_sem=walk_send.at[k],
            recv_sem=walk_recv.at[k],
            device_id={"walk": (my_walk + k) % m},
            device_id_type=MESH,
        )

    pl.when(me < n - 1)(lambda: pl.semaphore_wait(chain.at[2], 1))
    for k in range(1, m):
        walk_copy(k).start()

    def begin(g, _):
        acc[g] = jnp.dot(orb_t[me], chol_v[me * owned + g], preferred_element_type=jnp.float32)
        return _

    lax.fori_loop(0, last, begin, 0)
    acc_last[...] = jnp.dot(
        orb_t[me], chol_v[me * owned + last], preferred_element_type=jnp.float32
    )
    arrived[0] = products[my_walk]
    for k in range(1, m):
        walk_arrival(k).wait_recv()

    def term(v, _):
        block = chol_v[v].astype(jnp.float32)
        start = (v // owned) * share + v % owned
        for k in range(m):
            from_walk = (my_walk + k) % m
            for w in range(walkers):
                both = block * arrived[k, w].astype(jnp.float32)
                both = jnp.sum(both, axis=0, keepdims=True)
                part = both[:, :LANES]
                for lane in range(LANES, cols, LANES):
                    part = part + both[:, lane : lane + LANES]
                rows_v[pl.ds(start + (from_walk * walkers + w) * owned, 1), :] = part
        return _

    lax.fori_loop(0, vectors, term, 0)
    for b in range(terms.shape[0]):
        turned = rows_v[b * LANES : (b + 1) * LANES, :].T
        terms[b] = jnp.sum(turned, axis=0, keepdims=True)

    def take(g, k):
        chunk_copy(g, k).wait_recv()
        return jnp.dot(orb_t[xor(me, k, n)], chunks[k, g], preferred_element_type=jnp.float32)

    def arrival(i):
        return (half - 1 - i % (half - 1)) * 2 + i // (half - 1)

    steps = 2 * (half - 1)

    def add(g, k):
        if isinstance(g, int) and g == last:
            acc_last[...] += take(g, k)
        else:
            acc[g] += take(g, k)

    def add_some(g, start, stop):
        def step(i, _):
            add(g, arrival(i))
            return _

        lax.fori_loop(start, stop, step, 0)

    def finish(g):
        rounded[g] = (acc[g] + take(g, arrival(steps - 1))).astype(rounded.dtype)

    def term_copy(k):
        peer = xor(me, k, n)
        return pltpu.make_async_remote_copy(
            src_ref=terms.at[peer * share // LANES],
            dst_ref=terms_in.at[k],
            send_sem=term_send.at[k],
            recv_sem=term_recv.at[k],
            device_id={"orb": peer},
            device_id_type=MESH,
        )

    def sum_copy(k):
        peer = (my_walk + k) % m
        return pltpu.make_async_remote_copy(
            src_ref=sums,
            dst_ref=sums_in.at[m - k],
            send_sem=sum_send.at[k],
            recv_sem=sum_recv.at[m - k],
            device_id={"walk": peer},
            device_id_type=MESH,
        )

    def sum_arrival(k):
        return pltpu.make_async_remote_copy(
            src_ref=sums,
            dst_ref=sums_in.at[k],
            send_sem=sum_send.at[k],
            recv_sem=sum_recv.at[k],
            device_id={"walk": (my_walk + k) % m},
            device_id_type=MESH,
        )

    add(0, 1)
    add_some(0, 0, steps - 1)
    for k in range(1, n):
        term_copy(k).start()
    send_vector(last)
    finish(0)

    if owned > 2:
        def vector(g, _):
            add(g, 1)
            add_some(g, 0, steps - 1)
            finish(g)
            return _

        lax.fori_loop(1, owned - 1, vector, 0)

    def drain(g, _):
        def one(k, _):
            chunk_copy(g, k).wait_send()
            return _

        return lax.fori_loop(1, n, one, _)

    lax.fori_loop(0, last, drain, 0)
    for k in range(1, m):
        walk_copy(k).wait_send()
    for k in range(1, n):
        term_copy(k).wait_send()

    mine = terms[me * share // LANES]
    for k in range(1, n):
        term_copy(k).wait_recv()
        mine = mine + terms_in[k]
    sums[...] = mine
    add(last, 1)
    for k in range(1, m):
        sum_copy(k).start()
    add_some(last, 0, steps - 2)
    loads[3].wait()
    total = sums[...]
    for k in range(1, m):
        sum_arrival(k).wait_recv()
        total = total + sums_in[k]
    offset = (me * share) % LANES + my_walk * (walkers * owned)
    total = pltpu.roll(jnp.broadcast_to(total, (8, LANES)), (LANES - offset) % LANES, 1)
    for w in range(walkers):
        bias_out[w : w + 1, :] = total[:1, w * owned : (w + 1) * owned] - shift_v[...]
    for k in range(1, m):
        sum_copy(k).wait_send()
    add_some(last, steps - 2, steps - 1)

    def settle(i, _):
        chunk_copy(last, arrival(i)).wait_send()
        return _

    chunk_copy(last, 1).wait_send()
    lax.fori_loop(0, steps - 2, settle, 0)
    chunk_copy(last, final, dst=chunk_last).wait_recv()
    lax.fori_loop(steps - 2, steps, settle, 0)


def store(bias, rounded, acc_last, chunk_last, orb_last, bias_out, rotated, last_v, sems):
    last = rounded.shape[0]
    writes = [pltpu.make_async_copy(rounded.at[g], rotated.at[g], sems.at[g]) for g in range(last)]
    writes.append(pltpu.make_async_copy(last_v, rotated.at[last], sems.at[last]))
    writes.append(pltpu.make_async_copy(bias, bias_out, sems.at[last + 1]))
    for write in writes[:last]:
        write.start()
    last_v[...] = (
        acc_last[...]
        + jnp.dot(orb_last[...], chunk_last[...], preferred_element_type=jnp.float32)
    ).astype(last_v.dtype)
    for write in writes[last:]:
        write.start()
    for write in writes:
        write.wait()


def local(n, m, chol, orbitals, greens, shift):
    vectors, rows, cols = chol.shape
    owned = vectors // n
    walkers, occupied, _ = greens.shape
    bf16, f32 = jnp.bfloat16, jnp.float32
    dma = pltpu.SemaphoreType.DMA
    regular = pltpu.SemaphoreType.REGULAR
    any_space = pl.BlockSpec(memory_space=pl.ANY)
    vmem = pl.BlockSpec(memory_space=pltpu.VMEM)
    singles = n.bit_length() - 2
    packed = n * m * walkers * owned // LANES
    carried = pl.pallas_call(
        functools.partial(kernel, n, m),
        out_shape=(
            pltpu.VMEM((walkers, owned), f32),
            pltpu.VMEM((owned - 1, occupied, cols), bf16),
            pltpu.VMEM((occupied, cols), f32),
            pltpu.VMEM((rows, cols), bf16),
            pltpu.VMEM((occupied, rows), bf16),
        ),
        in_specs=[any_space] * 4,
        out_specs=(vmem,) * 5,
        scratch_shapes=[
            pltpu.VMEM((n, owned, rows, cols), bf16),
            pltpu.VMEM((singles, rows, cols), bf16),
            pltpu.VMEM(chol.shape, bf16),
            pltpu.VMEM(orbitals.shape, bf16),
            pltpu.VMEM((n, occupied, rows), bf16),
            pltpu.VMEM(greens.shape, bf16),
            pltpu.VMEM((m, walkers, rows, cols), bf16),
            pltpu.VMEM((m, walkers, rows, cols), bf16),
            pltpu.VMEM((owned - 1, occupied, cols), f32),
            pltpu.VMEM((packed * LANES, LANES), f32),
            pltpu.VMEM((packed, 1, LANES), f32),
            pltpu.VMEM((n, 1, LANES), f32),
            pltpu.VMEM((1, LANES), f32),
            pltpu.VMEM((m, 1, LANES), f32),
            pltpu.VMEM((1, owned), f32),
            dma((4 + singles,)),
            dma((n, owned)),
            dma((n, owned)),
            dma((m,)),
            dma((m,)),
            dma((n,)),
            dma((n,)),
            dma((m,)),
            dma((m,)),
            regular((n,)),
            regular((3,)),
        ],
        compiler_params=pltpu.CompilerParams(
            collective_id=0, has_side_effects=True, vmem_limit_bytes=56 * 2**20
        ),
    )(chol, orbitals, greens, shift.reshape(1, owned))
    return pl.pallas_call(
        store,
        out_shape=(
            jax.ShapeDtypeStruct((walkers, owned), f32),
            jax.ShapeDtypeStruct((owned, occupied, cols), bf16),
        ),
        in_specs=[vmem] * 5,
        out_specs=(any_space, any_space),
        scratch_shapes=[pltpu.VMEM((occupied, cols), bf16), dma((owned + 1,))],
        compiler_params=pltpu.CompilerParams(vmem_limit_bytes=8 * 2**20),
    )(*carried)


def solution(mesh):
    in_specs = (P(None, "orb", "walk"), P(), P("walk", None, None), P("orb"))
    out_specs = (P("walk", "orb"), P("orb", None, "walk"))
    body = functools.partial(local, mesh.shape["orb"], mesh.shape["walk"])
    return jax.shard_map(body, mesh=mesh, in_specs=in_specs, out_specs=out_specs, check_vma=False)
```

```python
import functools

import jax
import jax.numpy as jnp
from jax import lax
from jax.experimental import pallas as pl
from jax.experimental.pallas import tpu as pltpu
from jax.sharding import PartitionSpec as P

MESH = pl.DeviceIdType.MESH
LANES = 128


def xor(a, b, size):
    total, bit = 0, 1
    while bit < size:
        total = total + ((a // bit + b // bit) % 2) * bit
        bit *= 2
    return total


def low_bit(k):
    return k & -k


def ones(k):
    return bin(k).count("1")


def kernel(
    n, m, chol, orbitals, greens, shift,
    bias_out, rounded, acc_last, chunk_last, orb_last,
    chunks, first_v, chol_v, orb_v, orb_t, greens_v, products, arrived, acc,
    rows_v, terms, terms_in, sums, sums_in, shift_v,
    local_sem, send_sem, recv_sem, walk_send, walk_recv,
    term_send, term_recv, sum_send, sum_recv, heard, chain,
):
    me, my_walk = lax.axis_index("orb"), lax.axis_index("walk")
    vectors, rows, cols = chol.shape
    owned = vectors // n
    walkers = greens.shape[0]
    half = n // 2
    core = me % 2
    last, finals = owned - 1, (5, 3)
    leader = me == n - 1
    has_below, has_above = my_walk > 0, my_walk < m - 1
    bits = [1 << b for b in range(n.bit_length() - 1)]
    share = m * walkers * owned

    def is_set(bit):
        return (me // bit) % 2

    barrier = pltpu.get_barrier_semaphore()

    def greet_orb(bit):
        pl.semaphore_signal(barrier, inc=1, device_id={"orb": xor(me, bit, n)}, device_id_type=MESH)

    for bit in reversed(bits[1:]):
        pl.when(is_set(bit) == 0)(functools.partial(greet_orb, bit))
    greet_orb(1)

    def greet(other):
        pl.semaphore_signal(barrier, inc=1, device_id={"walk": other}, device_id_type=MESH)

    pl.when(leader & has_below)(lambda: greet(my_walk - 1))
    pl.when(leader & has_above)(lambda: greet(my_walk + 1))

    firsts = [
        pltpu.make_async_copy(chol.at[xor(me, bit, n) * owned], first_v.at[i], local_sem.at[4 + i])
        for i, bit in enumerate(bits[1:])
    ]
    for load in firsts:
        load.start()
    loads = [
        pltpu.make_async_copy(chol, chol_v, local_sem.at[0]),
        pltpu.make_async_copy(orbitals, orb_v, local_sem.at[1]),
        pltpu.make_async_copy(greens, greens_v, local_sem.at[2]),
        pltpu.make_async_copy(shift, shift_v, local_sem.at[3]),
    ]

    planes = (my_walk + m - 1) // m + (2 * m - 2 - my_walk) // m
    pl.semaphore_wait(barrier, 1 + sum(is_set(bit) for bit in bits[1:]) + me // (n - 1) * planes)

    def chunk_copy(g, k, src=None, dst=None):
        peer = xor(me, k, n)
        source = chol if isinstance(g, int) and g == 0 else chol_v
        return pltpu.make_async_remote_copy(
            src_ref=source.at[peer * owned + g] if src is None else src,
            dst_ref=chunks.at[k, g] if dst is None else dst,
            send_sem=send_sem.at[k, g],
            recv_sem=recv_sem.at[k, g],
            device_id={"orb": peer},
            device_id_type=MESH,
        )

    def place(k):
        return chunk_last.at[pl.ds(finals.index(k) * rows, rows)]

    def send_vector(g):
        for low in range(2):
            if low == 1:
                chunk_copy(g, 1).start()
            for high in range(1, half):
                if g == last and low == 1:
                    k = (half - high) * 2 + low
                    chunk_copy(g, k, dst=place(k) if k in finals else None).start()
                else:
                    chunk_copy(g, (high + core * (half - 2 * high)) * 2 + low).start()

    def tell(k):
        peer = xor(me, low_bit(k), n)
        pl.semaphore_signal(heard.at[k], inc=1, device_id={"orb": peer}, device_id_type=MESH)

    def hear(k):
        pl.semaphore_wait(heard.at[k], 1)

    def pass_along(k):
        for further in range(k + 1, n):
            if ones(further) == ones(k) + 1 and further - low_bit(further) == k:
                tell(further)

    def send_first(i, bit):
        firsts[i].wait()
        chunk_copy(0, bit, first_v.at[i]).start()

    for bit in reversed(bits[1:]):
        pl.when(is_set(bit) == 1)(functools.partial(tell, bit))
    for i, bit in enumerate(bits[1:]):
        pl.when(is_set(bit) == 1)(functools.partial(send_first, i, bit))
    for i, bit in enumerate(bits[1:]):
        pl.when(is_set(bit) == 0)(functools.partial(hear, bit))
        pl.when(is_set(bit) == 0)(functools.partial(send_first, i, bit))
        pass_along(bit)
    chunk_copy(0, 1).start()
    for low in range(2):
        for k in range(2 + low, n, 2):
            if ones(k) > 1:
                hear(k)
                pass_along(k)
                chunk_copy(0, k).start()
    for load in loads:
        load.start()
    loads[0].wait()
    for g in range(1, last):
        send_vector(g)

    def pass_on(i, other):
        pl.semaphore_signal(chain.at[i], inc=1, device_id={"walk": other}, device_id_type=MESH)

    pl.when(leader & has_below)(lambda: pl.semaphore_wait(chain.at[0], 1))
    pl.when(leader & has_above)(lambda: pass_on(0, my_walk + 1))
    pl.when(leader & has_above)(lambda: pl.semaphore_wait(chain.at[1], 1))
    pl.when(leader & has_below)(lambda: pass_on(1, my_walk - 1))

    @pl.when(leader)
    def _():
        for k in range(1, n):
            pl.semaphore_signal(
                chain.at[2], inc=1, device_id={"orb": xor(me, k, n)}, device_id_type=MESH
            )

    loads[1].wait()
    loads[2].wait()
    my_rows = orb_v[pl.ds(pl.multiple_of(me * rows, rows), rows), :]
    for w in range(walkers):
        for j in range(m):
            products[j, w] = jnp.dot(
                my_rows, greens_v[w, :, j * cols : (j + 1) * cols],
                preferred_element_type=jnp.float32,
            ).astype(products.dtype)

    def turn(s, _):
        orb_t[s] = orb_v[pl.ds(pl.multiple_of(s * rows, rows), rows), :].T
        return _

    lax.fori_loop(0, n, turn, 0)
    for i, k in enumerate(finals):
        orb_last[:, i * rows : (i + 1) * rows] = orb_t[xor(me, k, n)]

    def walk_copy(k):
        peer = (my_walk + k) % m
        return pltpu.make_async_remote_copy(
            src_ref=products.at[peer],
            dst_ref=arrived.at[m - k],
            send_sem=walk_send.at[k],
            recv_sem=walk_recv.at[m - k],
            device_id={"walk": peer},
            device_id_type=MESH,
        )

    def walk_arrival(k):
        return pltpu.make_async_remote_copy(
            src_ref=products.at[0],
            dst_ref=arrived.at[k],
            send_sem=walk_send.at[k],
            recv_sem=walk_recv.at[k],
            device_id={"walk": (my_walk + k) % m},
            device_id_type=MESH,
        )

    pl.when(me < n - 1)(lambda: pl.semaphore_wait(chain.at[2], 1))
    for k in range(1, m):
        walk_copy(k).start()

    def begin(g, _):
        acc[g] = jnp.dot(orb_t[me], chol_v[me * owned + g], preferred_element_type=jnp.float32)
        return _

    lax.fori_loop(0, last, begin, 0)
    acc_last[...] = jnp.dot(
        orb_t[me], chol_v[me * owned + last], preferred_element_type=jnp.float32
    )
    arrived[0] = products[my_walk]
    for k in range(1, m):
        walk_arrival(k).wait_recv()

    def term(v, _):
        block = chol_v[v].astype(jnp.float32)
        start = (v // owned) * share + v % owned
        for k in range(m):
            from_walk = (my_walk + k) % m
            for w in range(walkers):
                both = block * arrived[k, w].astype(jnp.float32)
                both = jnp.sum(both, axis=0, keepdims=True)
                part = both[:, :LANES]
                for lane in range(LANES, cols, LANES):
                    part = part + both[:, lane : lane + LANES]
                rows_v[pl.ds(start + (from_walk * walkers + w) * owned, 1), :] = part
        return _

    lax.fori_loop(0, vectors, term, 0)
    for b in range(terms.shape[0]):
        turned = rows_v[b * LANES : (b + 1) * LANES, :].T
        terms[b] = jnp.sum(turned, axis=0, keepdims=True)

    def take(g, k):
        chunk_copy(g, k).wait_recv()
        return jnp.dot(orb_t[xor(me, k, n)], chunks[k, g], preferred_element_type=jnp.float32)

    def arrival(i):
        return (half - 1 - i % (half - 1)) * 2 + i // (half - 1)

    steps = 2 * (half - 1)

    def add(g, k):
        if isinstance(g, int) and g == last:
            acc_last[...] += take(g, k)
        else:
            acc[g] += take(g, k)

    def add_some(g, start, stop):
        def step(i, _):
            add(g, arrival(i))
            return _

        lax.fori_loop(start, stop, step, 0)

    def finish(g):
        rounded[g] = (acc[g] + take(g, arrival(steps - 1))).astype(rounded.dtype)

    def term_copy(k):
        peer = xor(me, k, n)
        return pltpu.make_async_remote_copy(
            src_ref=terms.at[peer * share // LANES],
            dst_ref=terms_in.at[k],
            send_sem=term_send.at[k],
            recv_sem=term_recv.at[k],
            device_id={"orb": peer},
            device_id_type=MESH,
        )

    def sum_copy(k):
        peer = (my_walk + k) % m
        return pltpu.make_async_remote_copy(
            src_ref=sums,
            dst_ref=sums_in.at[m - k],
            send_sem=sum_send.at[k],
            recv_sem=sum_recv.at[m - k],
            device_id={"walk": peer},
            device_id_type=MESH,
        )

    def sum_arrival(k):
        return pltpu.make_async_remote_copy(
            src_ref=sums,
            dst_ref=sums_in.at[k],
            send_sem=sum_send.at[k],
            recv_sem=sum_recv.at[k],
            device_id={"walk": (my_walk + k) % m},
            device_id_type=MESH,
        )

    add(0, 1)
    add_some(0, 0, steps - 1)
    for k in range(1, n):
        term_copy(k).start()
    send_vector(last)
    finish(0)

    if owned > 2:
        def vector(g, _):
            add(g, 1)
            add_some(g, 0, steps - 1)
            finish(g)
            return _

        lax.fori_loop(1, owned - 1, vector, 0)

    def drain(g, _):
        def one(k, _):
            chunk_copy(g, k).wait_send()
            return _

        return lax.fori_loop(1, n, one, _)

    lax.fori_loop(0, last, drain, 0)
    for k in range(1, m):
        walk_copy(k).wait_send()
    for k in range(1, n):
        term_copy(k).wait_send()

    mine = terms[me * share // LANES]
    for k in range(1, n):
        term_copy(k).wait_recv()
        mine = mine + terms_in[k]
    sums[...] = mine
    add(last, 1)
    for k in range(1, m):
        sum_copy(k).start()
    add_some(last, 0, steps - 2)
    loads[3].wait()
    total = sums[...]
    for k in range(1, m):
        sum_arrival(k).wait_recv()
        total = total + sums_in[k]
    offset = (me * share) % LANES + my_walk * (walkers * owned)
    total = pltpu.roll(jnp.broadcast_to(total, (8, LANES)), (LANES - offset) % LANES, 1)
    for w in range(walkers):
        bias_out[w : w + 1, :] = total[:1, w * owned : (w + 1) * owned] - shift_v[...]
    for k in range(1, m):
        sum_copy(k).wait_send()

    def settle(i, _):
        chunk_copy(last, arrival(i)).wait_send()
        return _

    chunk_copy(last, 1).wait_send()
    lax.fori_loop(0, steps - 2, settle, 0)
    for k in finals:
        chunk_copy(last, k, dst=place(k)).wait_recv()
    lax.fori_loop(steps - 2, steps, settle, 0)


def store(bias, rounded, acc_last, chunk_last, orb_last, bias_out, rotated, last_v, sems):
    last = rounded.shape[0]
    height = last_v.shape[0] // 2
    writes = [pltpu.make_async_copy(rounded.at[g], rotated.at[g], sems.at[g]) for g in range(last)]
    writes.append(pltpu.make_async_copy(bias, bias_out, sems.at[last]))
    for write in writes:
        write.start()
    for i in range(2):
        span = pl.ds(i * height, height)
        last_v[span, :] = (
            acc_last[span, :]
            + jnp.dot(orb_last[span, :], chunk_last[...], preferred_element_type=jnp.float32)
        ).astype(last_v.dtype)
        writes.append(
            pltpu.make_async_copy(last_v.at[span], rotated.at[last, span], sems.at[last + 1 + i])
        )
        writes[-1].start()
    for write in writes:
        write.wait()


def local(n, m, chol, orbitals, greens, shift):
    vectors, rows, cols = chol.shape
    owned = vectors // n
    walkers, occupied, _ = greens.shape
    bf16, f32 = jnp.bfloat16, jnp.float32
    dma = pltpu.SemaphoreType.DMA
    regular = pltpu.SemaphoreType.REGULAR
    any_space = pl.BlockSpec(memory_space=pl.ANY)
    vmem = pl.BlockSpec(memory_space=pltpu.VMEM)
    singles = n.bit_length() - 2
    packed = n * m * walkers * owned // LANES
    carried = pl.pallas_call(
        functools.partial(kernel, n, m),
        out_shape=(
            pltpu.VMEM((walkers, owned), f32),
            pltpu.VMEM((owned - 1, occupied, cols), bf16),
            pltpu.VMEM((occupied, cols), f32),
            pltpu.VMEM((2 * rows, cols), bf16),
            pltpu.VMEM((occupied, 2 * rows), bf16),
        ),
        in_specs=[any_space] * 4,
        out_specs=(vmem,) * 5,
        scratch_shapes=[
            pltpu.VMEM((n, owned, rows, cols), bf16),
            pltpu.VMEM((singles, rows, cols), bf16),
            pltpu.VMEM(chol.shape, bf16),
            pltpu.VMEM(orbitals.shape, bf16),
            pltpu.VMEM((n, occupied, rows), bf16),
            pltpu.VMEM(greens.shape, bf16),
            pltpu.VMEM((m, walkers, rows, cols), bf16),
            pltpu.VMEM((m, walkers, rows, cols), bf16),
            pltpu.VMEM((owned - 1, occupied, cols), f32),
            pltpu.VMEM((packed * LANES, LANES), f32),
            pltpu.VMEM((packed, 1, LANES), f32),
            pltpu.VMEM((n, 1, LANES), f32),
            pltpu.VMEM((1, LANES), f32),
            pltpu.VMEM((m, 1, LANES), f32),
            pltpu.VMEM((1, owned), f32),
            dma((4 + singles,)),
            dma((n, owned)),
            dma((n, owned)),
            dma((m,)),
            dma((m,)),
            dma((n,)),
            dma((n,)),
            dma((m,)),
            dma((m,)),
            regular((n,)),
            regular((3,)),
        ],
        compiler_params=pltpu.CompilerParams(
            collective_id=0, has_side_effects=True, vmem_limit_bytes=56 * 2**20
        ),
    )(chol, orbitals, greens, shift.reshape(1, owned))
    return pl.pallas_call(
        store,
        out_shape=(
            jax.ShapeDtypeStruct((walkers, owned), f32),
            jax.ShapeDtypeStruct((owned, occupied, cols), bf16),
        ),
        in_specs=[vmem] * 5,
        out_specs=(any_space, any_space),
        scratch_shapes=[pltpu.VMEM((occupied, cols), bf16), dma((owned + 2,))],
        compiler_params=pltpu.CompilerParams(vmem_limit_bytes=8 * 2**20),
    )(*carried)


def solution(mesh):
    in_specs = (P(None, "orb", "walk"), P(), P("walk", None, None), P("orb"))
    out_specs = (P("walk", "orb"), P("orb", None, "walk"))
    body = functools.partial(local, mesh.shape["orb"], mesh.shape["walk"])
    return jax.shard_map(body, mesh=mesh, in_specs=in_specs, out_specs=out_specs, check_vma=False)
```

```python
import functools

import jax
import jax.numpy as jnp
from jax import lax
from jax.experimental import pallas as pl
from jax.experimental.pallas import tpu as pltpu
from jax.sharding import PartitionSpec as P

MESH = pl.DeviceIdType.MESH
LANES = 128


def xor(a, b, size):
    total, bit = 0, 1
    while bit < size:
        total = total + ((a // bit + b // bit) % 2) * bit
        bit *= 2
    return total


def low_bit(k):
    return k & -k


def ones(k):
    return bin(k).count("1")


def kernel(
    n, m, chol, orbitals, greens, shift,
    bias_out, rounded, acc_last, chunk_last, orb_last,
    chunks, first_v, chol_v, orb_v, orb_t, greens_v, products, arrived, acc,
    rows_v, terms, terms_in, sums, sums_in, shift_v,
    local_sem, send_sem, recv_sem, walk_send, walk_recv,
    term_send, term_recv, sum_send, sum_recv, heard, chain,
):
    me, my_walk = lax.axis_index("orb"), lax.axis_index("walk")
    vectors, rows, cols = chol.shape
    owned = vectors // n
    walkers = greens.shape[0]
    half = n // 2
    core = me % 2
    last, finals = owned - 1, (5, 3)
    leader = me == n - 1
    has_below, has_above = my_walk > 0, my_walk < m - 1
    bits = [1 << b for b in range(n.bit_length() - 1)]
    share = m * walkers * owned

    def is_set(bit):
        return (me // bit) % 2

    firsts = [
        pltpu.make_async_copy(chol.at[xor(me, bit, n) * owned], first_v.at[i], local_sem.at[4 + i])
        for i, bit in enumerate(bits[1:])
    ]
    for load in firsts:
        load.start()

    barrier = pltpu.get_barrier_semaphore()

    def greet_orb(bit):
        pl.semaphore_signal(barrier, inc=1, device_id={"orb": xor(me, bit, n)}, device_id_type=MESH)

    for bit in reversed(bits[1:]):
        pl.when(is_set(bit) == 0)(functools.partial(greet_orb, bit))
    greet_orb(1)

    def greet(other):
        pl.semaphore_signal(barrier, inc=1, device_id={"walk": other}, device_id_type=MESH)

    pl.when(leader & has_below)(lambda: greet(my_walk - 1))
    pl.when(leader & has_above)(lambda: greet(my_walk + 1))

    loads = [
        pltpu.make_async_copy(chol, chol_v, local_sem.at[0]),
        pltpu.make_async_copy(orbitals, orb_v, local_sem.at[1]),
        pltpu.make_async_copy(greens, greens_v, local_sem.at[2]),
        pltpu.make_async_copy(shift, shift_v, local_sem.at[3]),
    ]

    planes = (my_walk + m - 1) // m + (2 * m - 2 - my_walk) // m
    pl.semaphore_wait(barrier, 1 + sum(is_set(bit) for bit in bits[1:]) + me // (n - 1) * planes)

    def chunk_copy(g, k, src=None, dst=None):
        peer = xor(me, k, n)
        source = chol if isinstance(g, int) and g == 0 else chol_v
        return pltpu.make_async_remote_copy(
            src_ref=source.at[peer * owned + g] if src is None else src,
            dst_ref=chunks.at[k, g] if dst is None else dst,
            send_sem=send_sem.at[k, g],
            recv_sem=recv_sem.at[k, g],
            device_id={"orb": peer},
            device_id_type=MESH,
        )

    def place(k):
        return chunk_last.at[pl.ds(finals.index(k) * rows, rows)]

    def send_vector(g):
        for low in range(2):
            if low == 1:
                chunk_copy(g, 1).start()
            for high in range(1, half):
                if g == last and low == 1:
                    k = (half - high) * 2 + low
                    chunk_copy(g, k, dst=place(k) if k in finals else None).start()
                else:
                    chunk_copy(g, (high + core * (half - 2 * high)) * 2 + low).start()

    def tell(k):
        peer = xor(me, low_bit(k), n)
        pl.semaphore_signal(heard.at[k], inc=1, device_id={"orb": peer}, device_id_type=MESH)

    def hear(k):
        pl.semaphore_wait(heard.at[k], 1)

    def pass_along(k):
        for further in range(k + 1, n):
            if ones(further) == ones(k) + 1 and further - low_bit(further) == k:
                tell(further)

    def send_first(i, bit):
        firsts[i].wait()
        chunk_copy(0, bit, first_v.at[i]).start()

    for bit in reversed(bits[1:]):
        pl.when(is_set(bit) == 1)(functools.partial(tell, bit))
    for i, bit in enumerate(bits[1:]):
        pl.when(is_set(bit) == 1)(functools.partial(send_first, i, bit))
    for i, bit in enumerate(bits[1:]):
        pl.when(is_set(bit) == 0)(functools.partial(hear, bit))
        pl.when(is_set(bit) == 0)(functools.partial(send_first, i, bit))
        pass_along(bit)
    chunk_copy(0, 1).start()
    for low in range(2):
        for k in range(2 + low, n, 2):
            if ones(k) > 1:
                hear(k)
                pass_along(k)
                chunk_copy(0, k).start()
    for load in loads:
        load.start()
    loads[0].wait()
    for g in range(1, last):
        send_vector(g)

    def pass_on(i, other):
        pl.semaphore_signal(chain.at[i], inc=1, device_id={"walk": other}, device_id_type=MESH)

    pl.when(leader & has_below)(lambda: pl.semaphore_wait(chain.at[0], 1))
    pl.when(leader & has_above)(lambda: pass_on(0, my_walk + 1))
    pl.when(leader & has_above)(lambda: pl.semaphore_wait(chain.at[1], 1))
    pl.when(leader & has_below)(lambda: pass_on(1, my_walk - 1))

    @pl.when(leader)
    def _():
        for k in range(1, n):
            pl.semaphore_signal(
                chain.at[2], inc=1, device_id={"orb": xor(me, k, n)}, device_id_type=MESH
            )

    loads[1].wait()
    loads[2].wait()
    my_rows = orb_v[pl.ds(pl.multiple_of(me * rows, rows), rows), :]
    for w in range(walkers):
        for j in range(m):
            products[j, w] = jnp.dot(
                my_rows, greens_v[w, :, j * cols : (j + 1) * cols],
                preferred_element_type=jnp.float32,
            ).astype(products.dtype)

    def turn(s, _):
        orb_t[s] = orb_v[pl.ds(pl.multiple_of(s * rows, rows), rows), :].T
        return _

    lax.fori_loop(0, n, turn, 0)
    for i, k in enumerate(finals):
        orb_last[:, i * rows : (i + 1) * rows] = orb_t[xor(me, k, n)]

    def walk_copy(k):
        peer = (my_walk + k) % m
        return pltpu.make_async_remote_copy(
            src_ref=products.at[peer],
            dst_ref=arrived.at[m - k],
            send_sem=walk_send.at[k],
            recv_sem=walk_recv.at[m - k],
            device_id={"walk": peer},
            device_id_type=MESH,
        )

    def walk_arrival(k):
        return pltpu.make_async_remote_copy(
            src_ref=products.at[0],
            dst_ref=arrived.at[k],
            send_sem=walk_send.at[k],
            recv_sem=walk_recv.at[k],
            device_id={"walk": (my_walk + k) % m},
            device_id_type=MESH,
        )

    pl.when(me < n - 1)(lambda: pl.semaphore_wait(chain.at[2], 1))
    for k in range(1, m):
        walk_copy(k).start()

    def begin(g, _):
        acc[g] = jnp.dot(orb_t[me], chol_v[me * owned + g], preferred_element_type=jnp.float32)
        return _

    lax.fori_loop(0, last, begin, 0)
    acc_last[...] = jnp.dot(
        orb_t[me], chol_v[me * owned + last], preferred_element_type=jnp.float32
    )
    arrived[0] = products[my_walk]
    for k in range(1, m):
        walk_arrival(k).wait_recv()

    def term(v, _):
        block = chol_v[v].astype(jnp.float32)
        start = (v // owned) * share + v % owned
        for k in range(m):
            from_walk = (my_walk + k) % m
            for w in range(walkers):
                both = block * arrived[k, w].astype(jnp.float32)
                both = jnp.sum(both, axis=0, keepdims=True)
                part = both[:, :LANES]
                for lane in range(LANES, cols, LANES):
                    part = part + both[:, lane : lane + LANES]
                rows_v[pl.ds(start + (from_walk * walkers + w) * owned, 1), :] = part
        return _

    lax.fori_loop(0, vectors, term, 0)
    for b in range(terms.shape[0]):
        turned = rows_v[b * LANES : (b + 1) * LANES, :].T
        terms[b] = jnp.sum(turned, axis=0, keepdims=True)

    def take(g, k):
        chunk_copy(g, k).wait_recv()
        return jnp.dot(orb_t[xor(me, k, n)], chunks[k, g], preferred_element_type=jnp.float32)

    def arrival(i):
        return (half - 1 - i % (half - 1)) * 2 + i // (half - 1)

    steps = 2 * (half - 1)

    def add(g, k):
        if isinstance(g, int) and g == last:
            acc_last[...] += take(g, k)
        else:
            acc[g] += take(g, k)

    def add_some(g, start, stop):
        def step(i, _):
            add(g, arrival(i))
            return _

        lax.fori_loop(start, stop, step, 0)

    def finish(g):
        rounded[g] = (acc[g] + take(g, arrival(steps - 1))).astype(rounded.dtype)

    def term_copy(k):
        peer = xor(me, k, n)
        return pltpu.make_async_remote_copy(
            src_ref=terms.at[peer * share // LANES],
            dst_ref=terms_in.at[k],
            send_sem=term_send.at[k],
            recv_sem=term_recv.at[k],
            device_id={"orb": peer},
            device_id_type=MESH,
        )

    def sum_copy(k):
        peer = (my_walk + k) % m
        return pltpu.make_async_remote_copy(
            src_ref=sums,
            dst_ref=sums_in.at[m - k],
            send_sem=sum_send.at[k],
            recv_sem=sum_recv.at[m - k],
            device_id={"walk": peer},
            device_id_type=MESH,
        )

    def sum_arrival(k):
        return pltpu.make_async_remote_copy(
            src_ref=sums,
            dst_ref=sums_in.at[k],
            send_sem=sum_send.at[k],
            recv_sem=sum_recv.at[k],
            device_id={"walk": (my_walk + k) % m},
            device_id_type=MESH,
        )

    add(0, 1)
    add_some(0, 0, steps - 1)
    for k in range(1, n):
        term_copy(k).start()
    send_vector(last)
    finish(0)

    if owned > 2:
        def vector(g, _):
            add(g, 1)
            add_some(g, 0, steps - 1)
            finish(g)
            return _

        lax.fori_loop(1, owned - 1, vector, 0)

    def drain(g, _):
        def one(k, _):
            chunk_copy(g, k).wait_send()
            return _

        return lax.fori_loop(1, n, one, _)

    lax.fori_loop(0, last, drain, 0)
    for k in range(1, m):
        walk_copy(k).wait_send()
    for k in range(1, n):
        term_copy(k).wait_send()

    mine = terms[me * share // LANES]
    for k in range(1, n):
        term_copy(k).wait_recv()
        mine = mine + terms_in[k]
    sums[...] = mine
    add(last, 1)
    for k in range(1, m):
        sum_copy(k).start()
    add_some(last, 0, steps - 2)
    loads[3].wait()
    total = sums[...]
    for k in range(1, m):
        sum_arrival(k).wait_recv()
        total = total + sums_in[k]
    offset = (me * share) % LANES + my_walk * (walkers * owned)
    total = pltpu.roll(jnp.broadcast_to(total, (8, LANES)), (LANES - offset) % LANES, 1)
    for w in range(walkers):
        bias_out[w : w + 1, :] = total[:1, w * owned : (w + 1) * owned] - shift_v[...]
    for k in range(1, m):
        sum_copy(k).wait_send()

    def settle(i, _):
        chunk_copy(last, arrival(i)).wait_send()
        return _

    chunk_copy(last, 1).wait_send()
    lax.fori_loop(0, steps - 2, settle, 0)
    for k in finals:
        chunk_copy(last, k, dst=place(k)).wait_recv()
    lax.fori_loop(steps - 2, steps, settle, 0)


def store(bias, rounded, acc_last, chunk_last, orb_last, bias_out, rotated, last_v, sems):
    last = rounded.shape[0]
    height = last_v.shape[0] // 2
    writes = [pltpu.make_async_copy(rounded.at[g], rotated.at[g], sems.at[g]) for g in range(last)]
    writes.append(pltpu.make_async_copy(bias, bias_out, sems.at[last]))
    for write in writes:
        write.start()
    for i in range(2):
        span = pl.ds(i * height, height)
        last_v[span, :] = (
            acc_last[span, :]
            + jnp.dot(orb_last[span, :], chunk_last[...], preferred_element_type=jnp.float32)
        ).astype(last_v.dtype)
        writes.append(
            pltpu.make_async_copy(last_v.at[span], rotated.at[last, span], sems.at[last + 1 + i])
        )
        writes[-1].start()
    for write in writes:
        write.wait()


def local(n, m, chol, orbitals, greens, shift):
    vectors, rows, cols = chol.shape
    owned = vectors // n
    walkers, occupied, _ = greens.shape
    bf16, f32 = jnp.bfloat16, jnp.float32
    dma = pltpu.SemaphoreType.DMA
    regular = pltpu.SemaphoreType.REGULAR
    any_space = pl.BlockSpec(memory_space=pl.ANY)
    vmem = pl.BlockSpec(memory_space=pltpu.VMEM)
    singles = n.bit_length() - 2
    packed = n * m * walkers * owned // LANES
    carried = pl.pallas_call(
        functools.partial(kernel, n, m),
        out_shape=(
            pltpu.VMEM((walkers, owned), f32),
            pltpu.VMEM((owned - 1, occupied, cols), bf16),
            pltpu.VMEM((occupied, cols), f32),
            pltpu.VMEM((2 * rows, cols), bf16),
            pltpu.VMEM((occupied, 2 * rows), bf16),
        ),
        in_specs=[any_space] * 4,
        out_specs=(vmem,) * 5,
        scratch_shapes=[
            pltpu.VMEM((n, owned, rows, cols), bf16),
            pltpu.VMEM((singles, rows, cols), bf16),
            pltpu.VMEM(chol.shape, bf16),
            pltpu.VMEM(orbitals.shape, bf16),
            pltpu.VMEM((n, occupied, rows), bf16),
            pltpu.VMEM(greens.shape, bf16),
            pltpu.VMEM((m, walkers, rows, cols), bf16),
            pltpu.VMEM((m, walkers, rows, cols), bf16),
            pltpu.VMEM((owned - 1, occupied, cols), f32),
            pltpu.VMEM((packed * LANES, LANES), f32),
            pltpu.VMEM((packed, 1, LANES), f32),
            pltpu.VMEM((n, 1, LANES), f32),
            pltpu.VMEM((1, LANES), f32),
            pltpu.VMEM((m, 1, LANES), f32),
            pltpu.VMEM((1, owned), f32),
            dma((4 + singles,)),
            dma((n, owned)),
            dma((n, owned)),
            dma((m,)),
            dma((m,)),
            dma((n,)),
            dma((n,)),
            dma((m,)),
            dma((m,)),
            regular((n,)),
            regular((3,)),
        ],
        compiler_params=pltpu.CompilerParams(
            collective_id=0, has_side_effects=True, vmem_limit_bytes=56 * 2**20
        ),
    )(chol, orbitals, greens, shift.reshape(1, owned))
    return pl.pallas_call(
        store,
        out_shape=(
            jax.ShapeDtypeStruct((walkers, owned), f32),
            jax.ShapeDtypeStruct((owned, occupied, cols), bf16),
        ),
        in_specs=[vmem] * 5,
        out_specs=(any_space, any_space),
        scratch_shapes=[pltpu.VMEM((occupied, cols), bf16), dma((owned + 2,))],
        compiler_params=pltpu.CompilerParams(vmem_limit_bytes=8 * 2**20),
    )(*carried)


def solution(mesh):
    in_specs = (P(None, "orb", "walk"), P(), P("walk", None, None), P("orb"))
    out_specs = (P("walk", "orb"), P("orb", None, "walk"))
    body = functools.partial(local, mesh.shape["orb"], mesh.shape["walk"])
    return jax.shard_map(body, mesh=mesh, in_specs=in_specs, out_specs=out_specs, check_vma=False)
```
